16 devices in a mesh: dp: 2 (over y, z), cp: 8 (over x, core).
Axes of the slice: x: 4, y: 2, z: 1, core: 2. Of those that a mesh axis runs over, the one named last changes fastest.
The devices are a block of a 4x4x8 slice.
Arguments:
- x_in: bfloat16 [16, 512, 2048], P('dp', 'cp'), parts along dimension 0
- positions: int32 [1024], P(('dp', 'cp')), parts along dimension 0
- long_factor: float32 [32], replicated
- norm_gain: float32 [2048], replicated
- w_qkv: bfloat16 [2048, 6144], replicated
- w_out: bfloat16 [2048, 2048], replicated
- grad_y: bfloat16 [16, 512, 2048], P('dp', 'cp'), parts along dimension 0
Outputs:
- output 1: bfloat16 [16, 512, 2048], P('dp', 'cp'), parts along dimension 0
- output 2: bfloat16 [16, 512, 2048], P('dp', 'cp'), parts along dimension 0
- output 3: float32 [4096], P('dp'), parts along dimension 0
- output 4: float32 [4096, 6144], P('dp'), parts along dimension 0
- output 5: float32 [4096, 2048], P('dp'), parts along dimension 0
There are 2 independent parts. The reference program is written for one: setup_inputs(seed, part) draws one part's arguments, and reference() takes and returns one part's arrays. A program takes and returns all parts, laid end to end along the dimension named above; an argument that names none is the same for every part.
All inputs are finite; a program needn't handle non-finite values.
Results may differ from the reference program's by a relative error of at most 0.0147614.
Values are sent between devices in bfloat16 or wider.
A program may use at most 768 MiB of HBM per device.

```python
import math
import jax
import jax.numpy as jnp
from jax import lax

BATCH = 8
SEQ_LEN = 512
HIDDEN = 2048
HEADS = 32
HEAD_DIM = 64
HALF_DIM = HEAD_DIM // 2
WIDTH = HEADS * HEAD_DIM
NORM_EPS = 1e-5
MSCALE = math.sqrt(1.0 + math.log(32.0) / math.log(4096.0))
SCALE = 1.0 / math.sqrt(HEAD_DIM)
QK_GAIN = 1.6
MASK_VALUE = -1e30


def setup_inputs(seed: int = 0, part: int = 0) -> dict:
    part_keys = jax.random.split(jax.random.fold_in(jax.random.key(seed), part), 3)
    shared_keys = jax.random.split(jax.random.key(seed + 1), 4)
    x_in = jax.random.normal(part_keys[0], (BATCH, SEQ_LEN, HIDDEN), jnp.float32)
    gaps = jax.random.randint(part_keys[1], (SEQ_LEN,), 1, 3)
    positions = (jnp.cumsum(gaps) - 1).astype(jnp.int32)
    grad_y = jax.random.normal(part_keys[2], (BATCH, SEQ_LEN, HIDDEN), jnp.float32)
    long_factor = jnp.exp(jax.random.uniform(shared_keys[0], (HALF_DIM,), jnp.float32, 0.0, 2.5))
    norm_gain = jax.random.uniform(shared_keys[1], (HIDDEN,), jnp.float32, 0.5, 1.5)
    col_gain = jnp.concatenate([jnp.full((2 * WIDTH,), QK_GAIN, jnp.float32), jnp.ones((WIDTH,), jnp.float32)])
    w_qkv = jax.random.normal(shared_keys[2], (HIDDEN, 3 * WIDTH), jnp.float32) * (HIDDEN ** -0.5) * col_gain
    w_out = jax.random.normal(shared_keys[3], (WIDTH, HIDDEN), jnp.float32) * (WIDTH ** -0.5)
    return {'x_in': x_in.astype(jnp.bfloat16), 'positions': positions, 'long_factor': long_factor, 'norm_gain': norm_gain, 'w_qkv': w_qkv.astype(jnp.bfloat16), 'w_out': w_out.astype(jnp.bfloat16), 'grad_y': grad_y.astype(jnp.bfloat16)}


def rope_tables(positions, long_factor):
    exponent = jnp.arange(HALF_DIM, dtype=jnp.float32) * (2.0 / HEAD_DIM)
    inv_freq = 1.0 / (long_factor * jnp.power(10000.0, exponent))
    angles = positions.astype(jnp.float32)[:, None] * inv_freq[None, :]
    angle_pair = jnp.concatenate([angles, angles], axis=-1)
    return jnp.cos(angle_pair) * MSCALE, jnp.sin(angle_pair) * MSCALE


def rotate_half(values):
    return jnp.concatenate([-values[..., HALF_DIM:], values[..., :HALF_DIM]], axis=-1)


def head_attention(blocks):
    q_head, k_head, v_head = blocks
    scores = jnp.einsum('bqd,bkd->bqk', q_head.astype(jnp.float32), k_head.astype(jnp.float32)) * SCALE
    token_idx = jnp.arange(SEQ_LEN)
    scores = jnp.where(token_idx[None, :, None] >= token_idx[None, None, :], scores, MASK_VALUE)
    attn_probs = jax.nn.softmax(scores, axis=-1).astype(jnp.bfloat16)
    return jnp.einsum('bqk,bkd->bqd', attn_probs.astype(jnp.float32), v_head.astype(jnp.float32)).astype(jnp.bfloat16)


def heads_first(tensor):
    return jnp.transpose(tensor, (2, 0, 1, 3))


def block_forward(x_in, norm_gain, w_qkv32, w_out32, cos_tab, sin_tab):
    x_float = x_in.astype(jnp.float32)
    inv_rms = lax.rsqrt(jnp.mean(x_float * x_float, axis=-1, keepdims=True) + NORM_EPS)
    normed = (x_float * inv_rms * norm_gain).astype(jnp.bfloat16)
    qkv_all = jnp.dot(normed.reshape(BATCH * SEQ_LEN, HIDDEN).astype(jnp.float32), w_qkv32)
    qkv_all = qkv_all.reshape(BATCH, SEQ_LEN, 3, HEADS, HEAD_DIM)
    cos_b = cos_tab[None, :, None, :]
    sin_b = sin_tab[None, :, None, :]
    q_rot = (qkv_all[:, :, 0] * cos_b + rotate_half(qkv_all[:, :, 0]) * sin_b).astype(jnp.bfloat16)
    k_rot = (qkv_all[:, :, 1] * cos_b + rotate_half(qkv_all[:, :, 1]) * sin_b).astype(jnp.bfloat16)
    v_val = qkv_all[:, :, 2].astype(jnp.bfloat16)
    attn_out = lax.map(jax.checkpoint(head_attention), (heads_first(q_rot), heads_first(k_rot), heads_first(v_val)))
    attn_flat = jnp.transpose(attn_out, (1, 2, 0, 3)).reshape(BATCH * SEQ_LEN, WIDTH)
    proj = jnp.dot(attn_flat.astype(jnp.float32), w_out32).reshape(BATCH, SEQ_LEN, HIDDEN)
    return (x_float + proj).astype(jnp.bfloat16)


def reference(x_in, positions, long_factor, norm_gain, w_qkv, w_out, grad_y):
    cos_tab, sin_tab = rope_tables(positions, long_factor)

    def run(x_val, gain, w_first, w_second):
        return block_forward(x_val, gain, w_first, w_second, cos_tab, sin_tab)

    y_out, pullback = jax.vjp(run, x_in, norm_gain, w_qkv.astype(jnp.float32), w_out.astype(jnp.float32))
    grad_x, grad_gain, grad_wqkv, grad_wout = pullback(grad_y)
    return y_out, grad_x, grad_gain, grad_wqkv, grad_wout
```

```python
import functools
import math

import jax
import jax.numpy as jnp
from jax import lax
from jax.experimental import pallas as pl
from jax.experimental.pallas import tpu as pltpu
from jax.sharding import PartitionSpec as P

NORM_EPS = 1e-5
MSCALE = math.sqrt(1.0 + math.log(32.0) / math.log(4096.0))
MASK_VALUE = -1e30
F32, BF = jnp.float32, jnp.bfloat16
HD = 64
HALF = HD // 2
GW = 256
GH = GW // HD
NT = (((1,), (1,)), ((), ()))


def dot(a, b):
    return jnp.dot(a, b, preferred_element_type=F32)


def dot_nt(a, b):
    return lax.dot_general(a, b, NT, preferred_element_type=F32)


def rope_t(t, c, s):
    out = []
    for h in range(0, t.shape[0], HD):
        a, b = t[h:h + HALF], t[h + HALF:h + HD]
        out += [a * c - b * s, b * c + a * s]
    return jnp.concatenate(out, axis=0)


class Refs:
    pass


def projection(S, r_ref, gy_ref, ws, c, s):
    wq, wk, wv, wo = ws

    def q():
        S.qT[...] = rope_t(dot(r_ref[...], wq[...]).T, c[...], s[...]).astype(BF)

    def k():
        t = rope_t(dot(r_ref[...], wk[...]).T, c[...], s[...]).astype(BF)
        S.kT[...] = t
        S.kb[...] = t.T

    def v():
        t = dot(r_ref[...], wv[...]).astype(BF)
        S.vb[...] = t
        S.vT[...] = t.T

    def d():
        S.doT[...] = dot_nt(gy_ref[...], wo[...]).astype(BF).T

    return [q, k, v, d]


def attention(S, X, outs, c, s):
    o_out, oT_out, dq_out, dk_out, dv_out = outs
    T = S.kb.shape[0]
    HB = T // 2
    scale = 1.0 / math.sqrt(HD)
    kappa = scale * math.log2(math.e)
    keep = lax.broadcasted_iota(jnp.int32, (HB, HB), 0) <= lax.broadcasted_iota(jnp.int32, (HB, HB), 1)
    mxs = {}
    CH = 32

    def padrows(t, h):
        parts = []
        if h:
            parts.append(jnp.zeros((HD * h, t.shape[1]), BF))
        parts.append(t)
        if h < GH - 1:
            parts.append(jnp.zeros((HD * (GH - 1 - h), t.shape[1]), BF))
        return jnp.concatenate(parts, axis=0)

    def tiles():
        for qt in range(2):
            yield qt, HB * (qt + 1), slice(qt * HB, (qt + 1) * HB)

    def scores(h):
        SS, DP, hs = X.ss[h & 1], X.dd[h & 1], slice(HD * h, HD * h + HD)
        for qt, L, qs in tiles():
            st = dot(S.kb[:L, :], padrows(S.qT[hs, qs], h))
            diag = jnp.where(keep, st[L - HB:], MASK_VALUE)
            SS[L - HB:L, qs] = diag
            mx = jnp.max(diag, axis=0, keepdims=True)
            if qt:
                SS[:L - HB, qs] = st[:L - HB]
                mx = jnp.maximum(mx, jnp.max(st[:L - HB], axis=0, keepdims=True))
            mxs[h, qt] = mx * kappa
            DP[:L, qs] = dot(S.vb[:L, :], padrows(S.doT[hs, qs], h))

    def softmax(h):
        SS, PB = X.ss[h & 1], X.pp[h & 1]
        for qt, L, qs in tiles():
            acc = jnp.zeros((8, HB), F32)
            for i in range(0, L, CH):
                e = jnp.exp2(SS[i:i + CH, qs] * kappa - mxs[h, qt])
                acc = acc + jnp.sum(e.reshape(CH // 8, 8, HB), axis=0)
                SS[i:i + CH, qs] = e
            inv = 1.0 / jnp.sum(acc, axis=0, keepdims=True)
            for i in range(0, L, CH):
                p = SS[i:i + CH, qs] * inv
                SS[i:i + CH, qs] = p
                PB[i:i + CH, qs] = p.astype(BF)

    def d_scores(h):
        SS, DP, PB, DS = X.ss[h & 1], X.dd[h & 1], X.pp[h & 1], X.ds[h & 1]
        hs = slice(HD * h, HD * h + HD)
        for qt, L, qs in tiles():
            oh = dot(S.vT[hs, :L], PB[:L, qs])
            X.oT[hs, qs] = oh
            delta = jnp.sum(oh * S.doT[hs, qs].astype(F32), axis=0, keepdims=True)
            for i in range(0, L, CH):
                DS[i:i + CH, qs] = (SS[i:i + CH, qs] * (DP[i:i + CH, qs] - delta)).astype(BF)

    def grads(h):
        PB, DS = X.pp[h & 1], X.ds[h & 1]
        hs = slice(HD * h, HD * h + HD)
        X.dvT[hs, :HB] = dot_nt(S.doT[hs, :], PB[:HB, :])
        X.dvT[hs, HB:] = dot_nt(S.doT[hs, HB:], PB[HB:, HB:])
        for qt, L, qs in tiles():
            X.dqT[hs, qs] = dot(S.kT[hs, :L], DS[:L, qs])
        X.dkT[hs, :HB] = dot_nt(S.qT[hs, :], DS[:HB, :])
        X.dkT[hs, HB:] = dot_nt(S.qT[hs, HB:], DS[HB:, HB:])

    def finish():
        ot = X.oT[...].astype(BF)
        oT_out[...] = ot
        o_out[...] = ot.T
        cc, sc = c[...] * scale, s[...] * -scale
        dq_out[...] = rope_t(X.dqT[...], cc, sc).astype(BF).T
        dk_out[...] = rope_t(X.dkT[...], cc, sc).astype(BF).T
        dv_out[...] = X.dvT[...].astype(BF).T

    fp = functools.partial
    steps = [fp(scores, 0)]
    for h in range(GH):
        if h + 1 < GH:
            steps.append(fp(scores, h + 1))
        steps.append(fp(softmax, h))
        if h:
            steps.append(fp(grads, h - 1))
        steps.append(fp(d_scores, h))
    return steps + [fp(grads, GH - 1), finish]


def interleave(a, b):
    out, j = [], 0
    for i, f in enumerate(a):
        while j < len(b) and j * len(a) <= i * len(b):
            out.append(b[j])
            j += 1
        out.append(f)
    return out + b[j:]


def block_kernel(n_cp, n_seq, n_units, x_loc, gy_loc, tab_loc, gain, w_qkv, w_out,
                 x_all, gy_all, rT, o, oT, dq, dk, dv,
                 tab_all, cT, sT, wq, wk, wv, wo, xbuf, gybuf, rbuf, *rest):
    rest = list(rest)
    sets = []
    for _ in range(2):
        S = Refs()
        S.kb, S.vb, S.qT, S.kT, S.vT, S.doT = rest[:6]
        rest = rest[6:]
        sets.append(S)
    X = Refs()
    X.oT, X.dqT, X.dkT, X.dvT = rest[:4]
    X.ss, X.dd, X.pp, X.ds = rest[4:6], rest[6:8], rest[8:10], rest[10:12]
    send_sem, recv_sem, tab_send, tab_recv, w_sem, load_sem, put_sem = rest[12:]
    step = pl.program_id(0)
    n_steps = n_seq * n_units // 2
    spq = n_units // 2
    piece = x_loc.shape[1]
    T = n_cp * piece
    me = lax.axis_index('cp')
    chip, core = me // 2, me % 2
    n_chip = n_cp // 2
    right = lax.rem(chip + 1, n_chip) * 2 + core
    left = lax.rem(chip + n_chip - 1, n_chip) * 2 + core
    far = lax.rem(chip + 2, n_chip) * 2 + core
    mate = chip * 2 + (1 - core)
    XL, XR, XF, GL, GR, GF, XP, GP = range(8)

    def rows(q, dev):
        return pl.ds(pl.multiple_of(q * T + dev * piece, piece), piece)

    def send(src, dst, q, slot, to):
        pltpu.make_async_remote_copy(src_ref=src, dst_ref=dst, send_sem=send_sem.at[q], recv_sem=recv_sem.at[q, slot],
                                     device_id={'cp': to}, device_id_type=pl.DeviceIdType.MESH).start()

    def arrived(arr, q, slot, n=1):
        ref = arr.at[pl.ds(0, n * piece)]
        pltpu.make_async_copy(ref, ref, recv_sem.at[q, slot]).wait()

    def send_own(q):
        for loc, arr, from_left, from_right, from_mate in ((x_loc, x_all, XL, XR, XP), (gy_loc, gy_all, GL, GR, GP)):
            dst = arr.at[rows(q, me)]
            send(loc.at[q], dst, q, from_left, right)
            send(loc.at[q], dst, q, from_right, left)
            send(loc.at[q], dst, q, from_mate, mate)

    def relay_near(q):
        arrived(x_all, q, XL)
        src = x_all.at[rows(q, left)]
        send(src, src, q, XF, right)
        send(src, src, q, XP, mate)
        arrived(x_all, q, XR)
        src = x_all.at[rows(q, right)]
        send(src, src, q, XP, mate)
        arrived(gy_all, q, GR)
        src = gy_all.at[rows(q, right)]
        send(src, src, q, GF, left)
        send(src, src, q, GP, mate)
        arrived(gy_all, q, GL)
        src = gy_all.at[rows(q, left)]
        send(src, src, q, GP, mate)

    def relay_far(q):
        arrived(x_all, q, XF)
        src = x_all.at[rows(q, far)]
        send(src, src, q, XP, mate)
        arrived(gy_all, q, GF)
        src = gy_all.at[rows(q, far)]
        send(src, src, q, GP, mate)

    def load(q):
        arrived(x_all, q, XP, n_chip)
        arrived(gy_all, q, GP, n_chip)
        slot = lax.rem(q, 2)
        for p in range(n_cp):
            at = pl.ds(p * piece, piece)

            @pl.when(p == me)
            def _():
                pltpu.make_async_copy(x_loc.at[q], xbuf.at[at], load_sem.at[0]).start()
                pltpu.make_async_copy(gy_loc.at[q], gybuf.at[slot, at], load_sem.at[1]).start()

            @pl.when(p != me)
            def _():
                pltpu.make_async_copy(x_all.at[rows(q, p)], xbuf.at[at], load_sem.at[0]).start()
                pltpu.make_async_copy(gy_all.at[rows(q, p)], gybuf.at[slot, at], load_sem.at[1]).start()

    def put_own(q):
        at = pl.ds(pl.multiple_of(me * piece, piece), piece)
        return pltpu.make_async_copy(gybuf.at[lax.rem(q, 2), at], gy_all.at[rows(q, me)], put_sem)

    def normalize(q):
        pltpu.make_async_copy(xbuf, xbuf, load_sem.at[0]).wait()
        pltpu.make_async_copy(gybuf.at[0], gybuf.at[0], load_sem.at[1]).wait()
        put_own(q).start()
        slot = lax.rem(q, 2)

        def chunk(i, _):
            i = pl.multiple_of(i * 128, 128)
            for j in range(0, 128, 16):
                xf = xbuf[pl.ds(i + j, 16), :].astype(F32)
                inv = lax.rsqrt(jnp.mean(xf * xf, axis=1, keepdims=True) + NORM_EPS)
                rbuf[slot, pl.ds(i + j, 16), :] = (xf * inv * gain[...]).astype(BF)
            rT[:, pl.ds(i, 128)] = rbuf[slot, pl.ds(i, 128), :].T
            return 0

        lax.fori_loop(0, T // 128, chunk, 0)

    @pl.when(step == 0)
    def _():
        width = n_units * GW
        at = pl.multiple_of(core * width, width)
        loads = [pltpu.make_async_copy(w_qkv.at[:, pl.ds(pl.multiple_of(i * 2 * width + at, width), width)], buf, w_sem.at[i])
                 for i, buf in enumerate((wq, wk, wv))]
        loads.append(pltpu.make_async_copy(w_out.at[pl.ds(at, width), :], wo, w_sem.at[3]))
        for cp in loads:
            cp.start()
        barrier = pltpu.get_barrier_semaphore()
        for d in range(1, n_cp):
            pl.semaphore_signal(barrier, inc=1, device_id={'cp': lax.rem(me + d, n_cp)}, device_id_type=pl.DeviceIdType.MESH)
        pl.semaphore_wait(barrier, n_cp - 1)
        mine = pl.ds(pl.multiple_of(me * piece, piece), piece)
        for d in range(1, n_cp):
            pltpu.make_async_remote_copy(src_ref=tab_loc, dst_ref=tab_all.at[mine], send_sem=tab_send, recv_sem=tab_recv,
                                         device_id={'cp': lax.rem(me + d, n_cp)}, device_id_type=pl.DeviceIdType.MESH).start()
        send_own(0)
        tab_all[mine, :] = tab_loc[...]
        relay_near(0)
        send_own(1)
        relay_far(0)
        load(0)
        others = tab_all.at[pl.ds(0, (n_cp - 1) * piece)]
        pltpu.make_async_copy(others, others, tab_recv).wait()
        pltpu.make_async_copy(others, others, tab_send).wait()
        tab = tab_all[...].T
        cT[...] = tab[:HALF]
        sT[...] = tab[HALF:2 * HALF]
        normalize(0)
        for cp in loads:
            cp.wait()
        for f in projection(sets[0], rbuf.at[0], gybuf.at[0], [t.at[:, pl.ds(0, GW)] for t in (wq, wk, wv)] + [wo.at[pl.ds(0, GW), :]], cT, sT):
            f()

    seq = step // spq
    first = lax.rem(step, spq) == 0
    nxt = seq + 1

    @pl.when(first & (nxt < n_seq))
    def _():
        relay_near(nxt)

    @pl.when(first & (nxt + 1 < n_seq))
    def _():
        send_own(nxt + 1)

    def weights(u):
        at = pl.ds(pl.multiple_of(u * GW, GW), GW)
        return [t.at[:, at] for t in (wq, wk, wv)] + [wo.at[at, :]]

    def half_step(u, unit_next):
        cs = pl.ds(u * GW, GW)
        outs = [o.at[0, :, cs], oT.at[cs, :]] + [t.at[0, :, cs] for t in (dq, dk, dv)]
        un = lax.rem(unit_next, n_units)
        slot = lax.rem(unit_next // n_units, 2)
        for f in interleave(attention(sets[u], X, outs, cT, sT),
                            projection(sets[1 - u], rbuf.at[slot], gybuf.at[slot], weights(un), cT, sT)):
            f()

    half_step(0, step * 2 + 1)

    @pl.when(first & (nxt < n_seq))
    def _():
        relay_far(nxt)

    @pl.when(jnp.logical_not(first) & (nxt < n_seq))
    def _():
        put_own(seq).wait()
        load(nxt)
        normalize(nxt)

    half_step(1, step * 2 + 2)

    @pl.when(step == n_steps - 1)
    def _():
        put_own(n_seq - 1).wait()
        for q in range(n_seq):
            ref = x_all.at[pl.ds(0, (6 + 3 * n_chip - 4) * piece)]
            pltpu.make_async_copy(ref, ref, send_sem.at[q]).wait()


def block_call(x, gy, tab, gain, w_qkv, w_out, n_cp):
    n_seq, piece, D = x.shape
    T = n_cp * piece
    W = w_out.shape[0] // 2
    n_units = W // GW
    spq = n_units // 2
    n_steps = n_seq * spq
    V = pltpu.VMEM
    any_spec = pl.BlockSpec(memory_space=pl.ANY)
    whole = pl.BlockSpec(memory_space=pltpu.VMEM)
    act = pl.BlockSpec((1, T, 2 * GW), lambda j: (j // spq, 0, lax.rem(j, spq)))
    N = n_seq * T
    return pl.pallas_call(
        functools.partial(block_kernel, n_cp, n_seq, n_units),
        grid=(n_steps,),
        in_specs=[any_spec, any_spec, whole, whole, any_spec, any_spec],
        out_specs=[any_spec, any_spec, pl.BlockSpec((D, T), lambda j: (0, jnp.minimum((j + spq - 1) // spq, n_seq - 1))),
                   act, pl.BlockSpec((2 * GW, T), lambda j: (lax.rem(j, spq), j // spq)), act, act, act],
        out_shape=[jax.ShapeDtypeStruct((N, D), BF), jax.ShapeDtypeStruct((N, D), BF), jax.ShapeDtypeStruct((D, N), BF),
                   jax.ShapeDtypeStruct((n_seq, T, W), BF), jax.ShapeDtypeStruct((W, N), BF)]
        + [jax.ShapeDtypeStruct((n_seq, T, W), BF)] * 3,
        scratch_shapes=[V((T, 128), F32), V((HALF, T), F32), V((HALF, T), F32), V((D, W), BF), V((D, W), BF), V((D, W), BF), V((W, D), BF),
                        V((T, D), BF), V((2, T, D), BF), V((2, T, D), BF)]
        + ([V((T, GW), BF)] * 2 + [V((GW, T), BF)] * 4) * 2 + [V((GW, T), F32)] * 4 + [V((T, T), F32)] * 4 + [V((T, T), BF)] * 4
        + [pltpu.SemaphoreType.DMA((n_seq,)), pltpu.SemaphoreType.DMA((n_seq, 8)), pltpu.SemaphoreType.DMA, pltpu.SemaphoreType.DMA,
           pltpu.SemaphoreType.DMA((4,)), pltpu.SemaphoreType.DMA((2,)), pltpu.SemaphoreType.DMA],
        compiler_params=pltpu.CompilerParams(vmem_limit_bytes=63 * 1024 * 1024, collective_id=0, has_side_effects=True,
                                             dimension_semantics=("arbitrary",)),
        name="block",
    )(x, gy, tab, gain, w_qkv, w_out)


def wgrad_kernel(spec, *refs):
    M, N, K, BM, BK, n_g, n_in, copies, own, rhs_col = spec
    refs = list(refs)
    lhs, rhs = refs[:2] if M else (None, None)
    recvs = refs[2 if M else 0:][:len(copies)]
    outs = refs[n_in:]
    send, gs = (outs[0], outs[1:1 + n_g]) if M else (None, outs[:n_g])
    scr = outs[(1 if M else 0) + n_g:]
    core = lax.rem(lax.axis_index('cp'), 2)
    step = pl.program_id(0)
    PR, NSLOT = 128, 4
    if copies:
        bounce, in_sem, out_sem = scr[-3:]
        scr = scr[:-3]

    pieces = [(i, r) for i, c in enumerate(copies) for r in range(0, c[1], PR)]
    nk = K // BK if M else 1
    n_steps = (M // BM) * nk if M else 1

    def piece(p, out):
        i, r = pieces[p]
        g, rows, cols, row0, col0 = copies[i]
        buf = bounce.at[p % NSLOT, :, pl.ds(0, cols)]
        at_r, at_c = row0(1 - core), col0(1 - core)
        dst = gs[g].at[pl.ds(pl.multiple_of(at_r + r, PR), PR), pl.ds(pl.multiple_of(at_c, 128), cols)]
        if out:
            return pltpu.make_async_copy(buf, dst, out_sem.at[p % NSLOT])
        return pltpu.make_async_copy(recvs[i].at[pl.ds(r, PR), :], buf, in_sem.at[p % NSLOT])

    def copy_slot(p):
        if p < len(pieces):
            if p >= NSLOT:
                piece(p - NSLOT, True).wait()
            piece(p, False).start()
        if 0 <= p - 2 < len(pieces):
            piece(p - 2, False).wait()
            piece(p - 2, True).start()

    if not M:
        for p in range(len(pieces) + 2):
            copy_slot(p)
        for p in range(max(0, len(pieces) - NSLOT), len(pieces)):
            piece(p, True).wait()
        return

    wbuf, acc, w_sem, o_sem = scr
    m, k = step // nk, lax.rem(step, nk)
    slot = lax.rem(m, 2)

    def w_load(i):
        at = pl.ds(i * BK, BK)
        return pltpu.make_async_copy(rhs.at[at, pl.ds(rhs_col, N)], wbuf.at[at], w_sem.at[i])

    def put(mm, sl):
        g, row0, col0 = own
        src = acc.at[sl]
        at = pl.ds(pl.multiple_of(mm * BM, BM), BM)
        dst = gs[g].at[pl.ds(pl.multiple_of(row0(core) + mm * BM, BM), BM), pl.ds(pl.multiple_of(col0(core), 128), N)]
        return pltpu.make_async_copy(src, send.at[at], o_sem.at[sl, 0]), pltpu.make_async_copy(src, dst, o_sem.at[sl, 1])

    @pl.when(step == 0)
    def _():
        for i in range(nk):
            w_load(i).start()

    for s in range(n_steps):
        lo, hi = (len(pieces) + 2) * s // n_steps, (len(pieces) + 2) * (s + 1) // n_steps
        if hi > lo and copies:
            @pl.when(step == s)
            def _():
                for p in range(lo, hi):
                    copy_slot(p)

    for i in range(nk):
        @pl.when(step == i)
        def _():
            w_load(i).wait()

    @pl.when((k == 0) & (m >= 2))
    def _():
        for cp in put(m - 2, slot):
            cp.wait()

    w = wbuf.at[pl.ds(pl.multiple_of(k * BK, BK), BK)]

    @pl.when(k == 0)
    def _():
        acc[slot] = dot(lhs[...], w[...])

    @pl.when(k > 0)
    def _():
        acc[slot] += dot(lhs[...], w[...])

    @pl.when(k == nk - 1)
    def _():
        for cp in put(m, slot):
            cp.start()

    @pl.when(step == n_steps - 1)
    def _():
        for mm in range(max(0, M // BM - 2), M // BM):
            for cp in put(mm, mm % 2):
                cp.wait()
        for p in range(max(0, len(pieces) - NSLOT), len(pieces)):
            piece(p, True).wait()


def wgrad_call(name, lhs, rhs, n, rhs_col, own, gs, shapes, copies, BM=512, BK=1024):
    V = pltpu.VMEM
    any_spec = pl.BlockSpec(memory_space=pl.ANY)
    args, in_specs, out_specs, out_shape, scratch = [], [], [], [], []
    M = K = 0
    if lhs is not None:
        M, K = lhs.shape
        nk = K // BK
        args += [lhs, rhs]
        in_specs += [pl.BlockSpec((BM, BK), lambda j: (j // nk, lax.rem(j, nk))), any_spec]
        out_specs.append(any_spec)
        out_shape.append(jax.ShapeDtypeStruct((M, n), F32))
        scratch += [V((K, n), BF), V((2, BM, n), F32), pltpu.SemaphoreType.DMA((nk,)), pltpu.SemaphoreType.DMA((2, 2))]
    args += [c[0] for c in copies]
    in_specs += [any_spec] * len(copies)
    aliases = {}
    for i, g in enumerate(gs):
        if g is not None:
            aliases[len(args)] = len(out_shape)
            args.append(g)
            in_specs.append(any_spec)
        out_specs.append(any_spec)
        out_shape.append(jax.ShapeDtypeStruct(shapes[i], F32))
    if copies:
        wide = max(c[0].shape[1] for c in copies)
        scratch += [V((4, 128, wide), F32), pltpu.SemaphoreType.DMA((4,)), pltpu.SemaphoreType.DMA((4,))]
    spec = (M, n, K, BM, BK, len(gs), len(args), [(c[1], c[0].shape[0], c[0].shape[1], c[2], c[3]) for c in copies], own, rhs_col)
    return pl.pallas_call(
        functools.partial(wgrad_kernel, spec),
        grid=((M // BM) * (K // BK) if M else 1,),
        in_specs=in_specs, out_specs=out_specs, out_shape=out_shape, scratch_shapes=scratch,
        input_output_aliases=aliases,
        compiler_params=pltpu.CompilerParams(vmem_limit_bytes=40 * 1024 * 1024),
        cost_estimate=pl.CostEstimate(flops=2 * M * n * K, bytes_accessed=8 * M * n + 2 * (M * K + K * n), transcendentals=0),
        name=name,
    )(*args)


def solution(mesh):
    cp_size = mesh.shape['cp']
    swap = [(i, i ^ 1) for i in range(cp_size)]

    def device_fn(x_in, positions, long_factor, norm_gain, w_qkv, w_out, grad_y):
        batch, piece, hidden = x_in.shape
        width = w_out.shape[0]
        hw = width // 2
        me = lax.axis_index('cp')
        core = lax.rem(me, 2)
        half = long_factor.shape[0]
        exponent = jnp.arange(half, dtype=F32) * (1.0 / half)
        inv_freq = 1.0 / (long_factor * jnp.power(10000.0, exponent))
        angles = positions.astype(F32)[:, None] * inv_freq[None, :]
        tab = jnp.concatenate([jnp.cos(angles) * MSCALE, jnp.sin(angles) * MSCALE, jnp.zeros((piece, 128 - 2 * half), F32)], axis=1)
        _, gy_all, rT, o, oT, dq, dk, dv = block_call(x_in, grad_y, tab, norm_gain[None], w_qkv, w_out, cp_size)
        acts = (o, dq, dk, dv)
        mine = [lax.dynamic_slice_in_dim(t, me*piece, piece, 1) for t in acts]
        theirs = [lax.dynamic_slice_in_dim(t, (me ^ 1)*piece, piece, 1) for t in acts]
        got = [lax.ppermute(t, 'cp', swap) for t in theirs]

        def exchange(t):
            return lax.ppermute(t, 'cp', swap)

        zero = lambda c: 0
        at = lambda base: (lambda c: base + c * hw)
        flat = lambda t: t.reshape(-1, t.shape[2])
        s_qkv, s_out = (hidden, 3 * width), (width, hidden)
        send_o, g_out = wgrad_call('gw_out', oT, gy_all, hidden, 0, (0, at(0), zero), [None], [s_out], [])
        recv_o = exchange(send_o)
        send_v, g_qkv = wgrad_call('gw_v', rT, flat(dv), hw, 0, (0, zero, at(2 * width)), [None], [s_qkv], [])
        recv_v = exchange(send_v)
        send_k, g_qkv, g_out = wgrad_call('gw_k', rT, flat(dk), hw, 0, (0, zero, at(width)), [g_qkv, g_out], [s_qkv, s_out],
                                          [(recv_o, 1, at(0), zero)])
        recv_k = exchange(send_k)

        def join(a, b, axis):
            return jnp.concatenate([jnp.where(core == 0, a, b), jnp.where(core == 0, b, a)], axis=axis)

        o_own = join(mine[0], got[0], 2)
        d_qkv = jnp.concatenate([join(mine[i], got[i], 2) for i in (1, 2, 3)], axis=2)
        x_float = x_in.astype(F32)
        y_out = (x_float + jnp.einsum('bsh,hd->bsd', o_own, w_out, preferred_element_type=F32)).astype(BF)
        inv_rms = lax.rsqrt(jnp.mean(x_float * x_float, axis=-1, keepdims=True) + NORM_EPS)
        x_hat = x_float * inv_rms
        d_normed = jnp.einsum('bse,de->bsd', d_qkv, w_qkv, preferred_element_type=F32)
        g_gain = jnp.sum(d_normed * x_hat, axis=(0, 1))
        d = 1
        while d < cp_size:
            g_gain = g_gain + lax.ppermute(g_gain, 'cp', [(i, i ^ d) for i in range(cp_size)])
            d *= 2
        d_hat = d_normed * norm_gain
        dx_norm = inv_rms * (d_hat - x_hat * jnp.mean(d_hat * x_hat, axis=-1, keepdims=True))
        grad_x = (grad_y.astype(F32) + dx_norm).astype(BF)

        hq = hw // 2
        send_a, g_qkv = wgrad_call('gw_qa', rT, flat(dq), hq, 0, (0, zero, at(0)), [g_qkv], [s_qkv],
                                   [(recv_v, 0, zero, at(2 * width)), (recv_k, 0, zero, at(width))])
        recv_a = exchange(send_a)
        send_b, g_qkv = wgrad_call('gw_qb', rT, flat(dq), hq, hq, (0, zero, at(hq)), [g_qkv], [s_qkv], [])
        recv_b = exchange(send_b)
        (g_wqkv,) = wgrad_call('gw_end', None, None, 0, 0, None, [g_qkv], [s_qkv], [(recv_a, 0, zero, at(0)), (recv_b, 0, zero, at(hq))])
        return y_out, grad_x, g_gain, g_wqkv, g_out

    seq_spec = P('dp', 'cp', None)
    return jax.shard_map(device_fn, mesh=mesh, in_specs=(seq_spec, P(('dp', 'cp')), P(None), P(None), P(None, None), P(None, None), seq_spec), out_specs=(seq_spec, seq_spec, P('dp'), P('dp', None), P('dp', None)), check_vma=False)
```
